256 devices in a mesh: seq: 64 (over z, y, x_hi), head: 4 (over x_lo, core).
Axes of the slice: x: 4 (x_hi: 2, x_lo: 2; x = x_hi * 2 + x_lo), y: 4, z: 8, core: 2. Of those that a mesh axis runs over, the one named last changes fastest.
Arguments:
- queries: bfloat16 [8192, 4096], P('seq', 'head'), may hold values from -12 to 12
- keys: bfloat16 [8192, 2048], P('seq', 'head'), may hold values from -12 to 12
- values: bfloat16 [8192, 2048], P('seq', 'head'), may hold values from -6 to 6
- block_order: int32 [128], replicated, may hold values from 0 to 127, each once
Outputs:
- attn: bfloat16 [8192, 4096], P(('seq', 'head'))
- lse: float32 [16, 8192], P('head', 'seq')
The draws below stay inside these ranges and needn't reach their ends.
Inputs may be any that keep to these rules, and one draw needn't show every extreme that they name: device-order block j (rows j * 64 to j * 64 + 63) holds sequence positions block_order[j] * 64 onward, in order.
All inputs are finite; a program needn't handle non-finite values.
Results may differ from the reference program's by a relative error of at most 0.006.
Values may be sent and summed in bfloat16 or wider, within the bound.
No kernel may reach another device: no remote copies, remote signals or barrier semaphores. Data moves between devices by JAX's collectives and lax.ppermute only.
A program may use at most 128 MiB of HBM per device.

```python
import jax
import jax.numpy as jnp
from jax import lax

HQ = 16
KEY_VALUE_HEADS = 8
HEAD_SIZE = 256
S_DEV = 128
QUERY_GROUP = 2
BLK = 64
NB = 128
SEQUENCE_TOKENS = 8192
N_SEQ = 64


def draw_queries(key, part):
    base_offset = jax.random.truncated_normal(jax.random.fold_in(key, 1), -3.0, 3.0, (SEQUENCE_TOKENS, HQ * HEAD_SIZE), jnp.float32)
    return base_offset.astype(jnp.bfloat16)


def draw_keys(key, part):
    base_offset = jax.random.truncated_normal(jax.random.fold_in(key, 2), -3.0, 3.0, (SEQUENCE_TOKENS, KEY_VALUE_HEADS * HEAD_SIZE), jnp.float32)
    return base_offset.astype(jnp.bfloat16)


def level_of(stream_key, extent, shards, smallest, top_value):
    def one(axis_at, blocks):
        heights = jax.random.uniform(jax.random.fold_in(jax.random.fold_in(stream_key, 6), axis_at), (blocks,), jnp.float32, smallest / len(shards), top_value / len(shards))
        return jnp.repeat(jnp.exp(heights), extent[axis_at] // blocks).reshape((-1,) + (1,) * (len(extent) - axis_at - 1))

    factor_of = one(*shards[0])
    for cut in shards[1:]:
        factor_of = factor_of * one(*cut)
    return factor_of


def scatter_about(key, shape, spread, most, pieces=(), held_as=jnp.bfloat16):
    array = jax.random.normal(key, shape, jnp.float32) * spread
    if len(pieces) > 0:
        array = level_of(key, shape, pieces, -0.22, 0.18) * array
    return jnp.clip(array, min=-most, max=most).astype(held_as)


def setup_inputs(seed: int = 0) -> dict:
    key_of = jax.random.split(jax.random.key(seed), 5)
    queries = draw_queries(jax.random.fold_in(key_of[4], 71), 0)
    keys = draw_keys(jax.random.fold_in(key_of[4], 71), 0)
    values = scatter_about(key_of[2], (SEQUENCE_TOKENS, KEY_VALUE_HEADS * HEAD_SIZE), 1.0, 6.0, ((0, 64), (1, 4)))
    block_order = jax.random.permutation(key_of[3], NB).astype(jnp.int32)
    return {"queries": queries, "keys": keys, "values": values, "block_order": block_order}


def reference(queries, keys, values, block_order):
    rows = jnp.arange(SEQUENCE_TOKENS, dtype=jnp.int32)
    pos = (block_order[rows // BLK] * BLK + rows % BLK).astype(jnp.int32)
    query_head_count = queries.reshape(SEQUENCE_TOKENS, KEY_VALUE_HEADS, QUERY_GROUP, HEAD_SIZE)
    key_single = keys.reshape(SEQUENCE_TOKENS, KEY_VALUE_HEADS, HEAD_SIZE).astype(jnp.float32)
    value_single = values.reshape(SEQUENCE_TOKENS, KEY_VALUE_HEADS, HEAD_SIZE).astype(jnp.float32)
    scale = HEAD_SIZE ** -0.5

    def one_block(index):
        start = (index * S_DEV).astype(jnp.int32)
        query_block = lax.dynamic_slice_in_dim(query_head_count, start, S_DEV, 0).astype(jnp.float32)
        query_pos = lax.dynamic_slice_in_dim(pos, start, S_DEV, 0)
        scores = jnp.einsum('qhgd,khd->hgqk', query_block, key_single) * scale
        allowed = pos[None, :] <= query_pos[:, None]
        scores = jnp.where(allowed, scores, -1e30)
        row_max = jnp.max(scores, axis=-1)
        weights = jnp.where(allowed, jnp.exp(scores - row_max[..., None]), 0.0)
        total = jnp.sum(weights, axis=-1)
        rounded = lax.optimization_barrier(weights.astype(jnp.bfloat16))
        summed = jnp.einsum('hgqk,khd->qhgd', rounded.astype(jnp.float32), value_single)
        output = summed / jnp.transpose(total, (2, 0, 1))[..., None]
        return output.reshape(S_DEV, HQ * HEAD_SIZE).astype(jnp.bfloat16), (row_max + jnp.log(total)).reshape(HQ, S_DEV)

    outputs, sums = lax.map(one_block, jnp.arange(N_SEQ, dtype=jnp.int32))
    attn = outputs.reshape(SEQUENCE_TOKENS, HQ * HEAD_SIZE)
    lse = jnp.transpose(sums, (1, 0, 2)).reshape(HQ, SEQUENCE_TOKENS)
    return attn, lse
```

```python
import functools

import jax
import jax.numpy as jnp
from jax import lax
from jax.experimental import pallas as pl
from jax.experimental.pallas import tpu as pltpu
from jax.sharding import Mesh
from jax.sharding import PartitionSpec as P


D = 256
BLK = 64
NZ, NY = 8, 4
SCALE = D**-0.5
LOG2E = 1.4426950408889634
NEG = -1e30
KT = 512
WIDE = 640

CHUNKS = [(0, 0), (0, 1)]
for _k in (1, 2, 3):
    CHUNKS += [(-_k, 0), (_k, 0), (-_k, 1), (_k, 1)]
CHUNKS += [(4, 0), (4, 1)]
TARGETS = (2, 1, 3, 0)

RANK, KPOS, QPOS, QNUM, QROW = 0, 32, 64, 80, 96


def shift_z(x, step):
    return lax.ppermute(x, "z", [(i, (i + step) % NZ) for i in range(NZ)])


def shift_y(x, step):
    return lax.ppermute(x, "y", [(i, (i + step) % NY) for i in range(NY)])


def cross(x, step):
    pairs = [
        (z * 2 + h, ((z + step) % NZ) * 2 + 1 - h) for z in range(NZ) for h in range(2)
    ]
    return lax.ppermute(x, ("z", "xh"), pairs)


def table_kernel(at_ref, order_ref, out_ref):
    z, y, xh = at_ref[0], at_ref[1], at_ref[2]

    def key_pos(j):
        step, other = CHUNKS[j // 2]
        zz = lax.rem(z + (step + NZ), NZ)
        hh = 1 - xh if other else xh
        return order_ref[((zz * NY + y) * 2 + hh) * 2 + j % 2]

    pos = [key_pos(j) for j in range(32)]
    rank = [jnp.int32(0)] * 32
    for i in range(32):
        for j in range(i):
            less = (pos[i] < pos[j]).astype(jnp.int32)
            rank[j] = rank[j] + less
            rank[i] = rank[i] + (1 - less)
    for j in range(32):
        out_ref[RANK + j] = rank[j]
        out_ref[KPOS + rank[j]] = pos[j]
    for g in range(8):
        yy = lax.rem(y + TARGETS[g // 2], NY)
        out_ref[QROW + g] = yy * 2 + g % 2
        for b in range(2):
            p = order_ref[((z * NY + yy) * 2 + g % 2) * 2 + b]
            count = jnp.int32(0)
            for j in range(32):
                count = count + (pos[j] <= p).astype(jnp.int32)
            out_ref[QPOS + 2 * g + b] = p
            out_ref[QNUM + 2 * g + b] = count


def table(at, order):
    return pl.pallas_call(
        table_kernel,
        out_shape=jax.ShapeDtypeStruct((128,), jnp.int32),
        in_specs=[pl.BlockSpec(memory_space=pltpu.SMEM)] * 2,
        out_specs=pl.BlockSpec(memory_space=pltpu.SMEM),
        name="table",
    )(at, order)


def attend_kernel(tab_ref, q_ref, *refs):
    kv_refs, out_refs = refs[:16], refs[16:20]
    ks, vs, scores, acc = refs[20:]
    for j in range(32):
        at = pl.multiple_of(tab_ref[RANK + j] * BLK, BLK)
        rows = pl.ds((j % 2) * BLK, BLK)
        ks[pl.ds(at, BLK), :] = kv_refs[j // 2][rows, :D]
        vs[pl.ds(at, BLK), :] = kv_refs[j // 2][rows, D:]

    row = lax.broadcasted_iota(jnp.int32, (256, 1), 0)
    within = row % BLK
    second = (row // BLK) % 2 == 1
    lane = lax.broadcasted_iota(jnp.int32, (1, KT), 1)
    lane_block = lane // BLK
    slot = lax.broadcasted_iota(jnp.int32, (128, 128), 1)

    for g in range(8):
        q = q_ref[tab_ref[QROW + g]]
        q = jnp.concatenate([q[:, :D], q[:, D:]], axis=0)
        p0, p1 = tab_ref[QPOS + 2 * g], tab_ref[QPOS + 2 * g + 1]
        row_pos = jnp.where(second, p1, p0) * BLK + within
        count = jnp.maximum(tab_ref[QNUM + 2 * g], tab_ref[QNUM + 2 * g + 1])
        tiles = (count + (KT // BLK - 1)) // (KT // BLK)

        def score(t, top):
            at = pl.multiple_of(t * KT, KT)
            s = lax.dot_general(
                q, ks[pl.ds(at, KT), :], (((1,), (1,)), ((), ())),
                preferred_element_type=jnp.float32,
            )
            block = jnp.zeros_like(lane)
            for b in range(KT // BLK):
                block = jnp.where(lane_block == b, tab_ref[KPOS + t * (KT // BLK) + b], block)
            col_pos = block * BLK + lane % BLK
            s = jnp.where(col_pos <= row_pos, s, NEG)
            scores[:, pl.ds(at, KT)] = s
            for i in range(KT // 128):
                top = jnp.maximum(top, s[:, i * 128 : (i + 1) * 128])
            return top

        top = lax.fori_loop(0, tiles, score, jnp.full((256, 128), NEG, jnp.float32))
        top = jnp.max(top, axis=1, keepdims=True)
        base = jnp.where(top > 0.5 * NEG, top, 0.0)
        acc[...] = jnp.zeros_like(acc)

        def weigh(t, total):
            at = pl.multiple_of(t * KT, KT)
            w = jnp.exp2((scores[:, pl.ds(at, KT)] - base) * (SCALE * LOG2E))
            for i in range(KT // 128):
                total = total + w[:, i * 128 : (i + 1) * 128]
            acc[...] += jnp.dot(
                w.astype(jnp.bfloat16), vs[pl.ds(at, KT), :], preferred_element_type=jnp.float32
            )
            return total

        total = lax.fori_loop(0, tiles, weigh, jnp.zeros((256, 128), jnp.float32))
        total = jnp.sum(total, axis=1, keepdims=True)
        some = total > 0.0
        safe = jnp.where(some, total, 1.0)
        o = (acc[...] / safe).astype(jnp.bfloat16)
        lse = jnp.where(some, base * SCALE + jnp.log(safe), NEG)
        out = out_refs[g // 2]
        rows = pl.ds((g % 2) * 128, 128)
        out[rows, :D] = o[:128]
        out[rows, D : 2 * D] = o[128:]
        high = lse.astype(jnp.bfloat16).astype(jnp.float32)
        mid = (lse - high).astype(jnp.bfloat16).astype(jnp.float32)
        low = lse - high - mid
        parts = jnp.zeros((128, 128), jnp.float32)
        for i, part in enumerate((high, mid, low)):
            parts = jnp.where(slot == i, part[:128], parts)
            parts = jnp.where(slot == 64 + i, part[128:], parts)
        out[rows, 2 * D :] = parts.astype(jnp.bfloat16)


def attend_blocks(tab, q, chunks):
    return pl.pallas_call(
        attend_kernel,
        out_shape=[jax.ShapeDtypeStruct((256, WIDE), jnp.bfloat16)] * 4,
        in_specs=[pl.BlockSpec(memory_space=pltpu.SMEM)]
        + [pl.BlockSpec(memory_space=pltpu.VMEM)] * 17,
        out_specs=[pl.BlockSpec(memory_space=pltpu.VMEM)] * 4,
        scratch_shapes=[
            pltpu.VMEM((2048, D), jnp.bfloat16),
            pltpu.VMEM((2048, D), jnp.bfloat16),
            pltpu.VMEM((256, 2048), jnp.float32),
            pltpu.VMEM((256, D), jnp.float32),
        ],
        compiler_params=pltpu.CompilerParams(vmem_limit_bytes=40 << 20),
        cost_estimate=pl.CostEstimate(
            flops=4 * 2048 * 2048 * D, bytes_accessed=4 << 20, transcendentals=2048 * 2048
        ),
        name="attend",
    )(tab, q, *chunks)


def combine_kernel(*refs):
    part_refs, out_ref, lse_ref = refs[:4], refs[4], refs[5]
    slot = lax.broadcasted_iota(jnp.int32, (256, 128), 1)
    columns = jnp.zeros((256, 128), jnp.float32)
    for h in range(2):
        lses = []
        for r in part_refs:
            x = r[:, 2 * D :].astype(jnp.float32)
            lses.append(x[:, 64 * h : 64 * h + 1] + x[:, 64 * h + 1 : 64 * h + 2] + x[:, 64 * h + 2 : 64 * h + 3])
        top = functools.reduce(jnp.maximum, lses)
        ws = [jnp.exp(x - top) for x in lses]
        total = functools.reduce(jnp.add, ws)
        o = jnp.zeros((256, D), jnp.float32)
        for w, r in zip(ws, part_refs):
            o = o + (w / total) * r[:, h * D : (h + 1) * D].astype(jnp.float32)
        out_ref[:, h * D : (h + 1) * D] = o.astype(jnp.bfloat16)
        columns = jnp.where(slot == h, top + jnp.log(total), columns)
    lse_ref[...] = columns


def combine(parts):
    return pl.pallas_call(
        combine_kernel,
        out_shape=[
            jax.ShapeDtypeStruct((256, 2 * D), jnp.bfloat16),
            jax.ShapeDtypeStruct((256, 128), jnp.float32),
        ],
        in_specs=[pl.BlockSpec(memory_space=pltpu.VMEM)] * 4,
        out_specs=[pl.BlockSpec(memory_space=pltpu.VMEM)] * 2,
        name="combine",
    )(*parts)


def local(queries, keys, values, block_order):
    z, y, xh = lax.axis_index("z"), lax.axis_index("y"), lax.axis_index("xh")
    tab = table(jnp.stack([z, y, xh]).astype(jnp.int32), block_order)

    halves = jnp.stack([queries[:, : 2 * D], queries[:, 2 * D :]])
    to_send = jnp.broadcast_to(halves[None], (NY, 2, 128, 2 * D)).reshape(2 * NY, 128, 2 * D)
    q = lax.all_to_all(to_send, ("y", "xh"), split_axis=0, concat_axis=0, tiled=True)

    def half(which):
        return jnp.concatenate(
            [lax.dynamic_slice_in_dim(a, which * D, D, 1) for a in (keys, values)], axis=1
        )

    mine, theirs = half(xh), half(1 - xh)
    chunks = [mine, cross(theirs, 0)]
    a_up, a_down = shift_z(mine, 1), shift_z(mine, -1)
    b_up, b_down = cross(theirs, 1), cross(theirs, -1)
    chunks += [a_up, a_down, b_up, b_down]
    for _ in range(2):
        a_up, a_down = shift_z(a_up, 1), shift_z(a_down, -1)
        b_up, b_down = shift_z(b_up, 1), shift_z(b_down, -1)
        chunks += [a_up, a_down, b_up, b_down]
    chunks += [shift_z(a_up, 1), shift_z(b_down, -1)]

    partials = attend_blocks(tab, q, chunks)
    parts = [shift_y(p, t) if t else p for p, t in zip(partials, TARGETS)]
    out, columns = combine(parts)

    recv = lax.all_to_all(
        out.reshape(8, 32, 2 * D), ("xh", "xl", "c"), split_axis=0, concat_axis=0, tiled=True
    )
    attn = recv.reshape(2, 4, 32, 2 * D).transpose(2, 1, 0, 3).reshape(32, 16 * D)

    lse = columns[:, :2].T.reshape(2, 2, 128)
    own = lax.dynamic_index_in_dim(lse, xh, 1, keepdims=False)
    give = lax.dynamic_index_in_dim(lse, 1 - xh, 1, keepdims=False)
    take = lax.ppermute(give, "xh", [(0, 1), (1, 0)])
    first = jnp.where(xh == 0, own, take)
    last = jnp.where(xh == 0, take, own)
    return attn, jnp.concatenate([first, last], axis=0)


def solution(mesh):
    fine = Mesh(mesh.devices.reshape(NZ, NY, 2, 2, 2), ("z", "y", "xh", "xl", "c"))
    seq, head = ("z", "y", "xh"), ("xl", "c")
    in_specs = (P(seq, head), P(seq, head), P(seq, head), P())
    out_specs = (P(seq + head, None), P(head, seq))
    return jax.shard_map(local, mesh=fine, in_specs=in_specs, out_specs=out_specs, check_vma=False)
```

```python
import functools

import jax
import jax.numpy as jnp
from jax import lax
from jax.experimental import pallas as pl
from jax.experimental.pallas import tpu as pltpu
from jax.sharding import Mesh
from jax.sharding import PartitionSpec as P


D = 256
BLK = 64
NZ, NY = 8, 4
SCALE = D**-0.5
LOG2E = 1.4426950408889634
NEG = -1e30
ROWS = 272

CHUNKS = [(0, 0), (0, 1)]
for _k in (1, 2, 3):
    CHUNKS += [(-_k, 0), (_k, 0), (-_k, 1), (_k, 1)]
CHUNKS += [(4, 0), (4, 1)]
SPLIT = ((2, 1, 3, 0),)

def shift_z(x, step):
    return lax.ppermute(x, "z", [(i, (i + step) % NZ) for i in range(NZ)])


def shift_y(x, step):
    return lax.ppermute(x, "y", [(i, (i + step) % NY) for i in range(NY)])


def cross(x, step):
    pairs = [
        (z * 2 + h, ((z + step) % NZ) * 2 + 1 - h) for z in range(NZ) for h in range(2)
    ]
    return lax.ppermute(x, ("z", "xh"), pairs)


def attend_kernel(steps, order_ref, q_ref, *refs):
    kv_refs, out_refs = refs[:16], refs[16 : 16 + len(steps)]
    scores, weights, bias, lses = refs[16 + len(steps) :]
    z, y, xh = lax.axis_index("z"), lax.axis_index("y"), lax.axis_index("xh")
    columns = []
    for dz, other in CHUNKS:
        zz = lax.rem(z + (dz + NZ), NZ)
        block = ((zz * NY + y) * 2 + (1 - xh if other else xh)) * 2
        lane = lax.broadcasted_iota(jnp.int32, (8, 128), 1)
        columns.append(jnp.where(lane < BLK, order_ref[block], order_ref[block + 1]))
    for step, out_ref in zip(steps, out_refs):
        owner = lax.rem(y + step, NY)
        attend_rows(
            step, owner, (z * NY + owner) * 4, columns, order_ref, q_ref, kv_refs, out_ref,
            scores, weights, bias, lses,
        )


def attend_rows(
    step, yy, first, columns, order_ref, q_ref, kv_refs, out_ref, scores, weights, bias, lses
):
    row_pos = [order_ref[first + i] for i in range(4)]
    for j in range(16):
        for i in range(4):
            bias[8 * i : 8 * i + 8, j * 128 : (j + 1) * 128] = jnp.where(
                columns[j] <= row_pos[i], 0.0, NEG
            )

    def score(g):
        q = q_ref[yy * 2 + g]
        q = jnp.concatenate([q[:, :D], q[:, D:]], axis=0)
        tops = [jnp.full((BLK, 128), NEG, jnp.float32) for _ in range(4)]
        for p in range(8):
            k = jnp.concatenate([kv_refs[2 * p][:, :D], kv_refs[2 * p + 1][:, :D]], axis=0)
            s = lax.dot_general(q, k, (((1,), (1,)), ((), ())), preferred_element_type=jnp.float32)
            if step == 0 and p == 0:
                row = lax.broadcasted_iota(jnp.int32, (256, 1), 0)
                at = jnp.where((row // BLK) % 2 == 1, row_pos[2 * g + 1], row_pos[2 * g]) * BLK + row % BLK
                lane = lax.broadcasted_iota(jnp.int32, (1, 128), 1)
                cols = [columns[j][:1] * BLK + lane % BLK for j in range(2)]
                s = jnp.where(jnp.concatenate(cols, axis=1) <= at, s, NEG)
            for r in range(4):
                part = s[r * BLK : (r + 1) * BLK]
                if not (step == 0 and p == 0):
                    i = 2 * g + r % 2
                    part = part + bias[8 * i : 8 * i + 1, p * D : (p + 1) * D]
                scores[g, r * BLK : (r + 1) * BLK, p * D : (p + 1) * D] = part
                tops[r] = jnp.maximum(tops[r], jnp.maximum(part[:, :128], part[:, 128:]))
        return [jnp.max(t, axis=1, keepdims=True) for t in tops]

    def weigh(g, tops):
        totals, bases = [], []
        for r in range(4):
            base = jnp.where(tops[r] > 0.5 * NEG, tops[r], 0.0)
            total = jnp.zeros((BLK, 128), jnp.float32)
            for p in range(8):
                w = jnp.exp2((scores[g, r * BLK : (r + 1) * BLK, p * D : (p + 1) * D] - base) * (SCALE * LOG2E))
                total = total + (w[:, :128] + w[:, 128:])
                weights[g, r * BLK : (r + 1) * BLK, p * D : (p + 1) * D] = w.astype(jnp.bfloat16)
            totals.append(jnp.sum(total, axis=1, keepdims=True))
            bases.append(base)
        return jnp.concatenate(totals, axis=0), jnp.concatenate(bases, axis=0)

    def gather(g, total, base):
        acc = jnp.zeros((256, D), jnp.float32)
        for p in range(8):
            v = jnp.concatenate([kv_refs[2 * p][:, D:], kv_refs[2 * p + 1][:, D:]], axis=0)
            acc = acc + jnp.dot(weights[g, :, p * D : (p + 1) * D], v, preferred_element_type=jnp.float32)
        some = total > 0.0
        safe = jnp.where(some, total, 1.0)
        o = (acc / safe).astype(jnp.bfloat16)
        out_ref[g * 128 : (g + 1) * 128, :D] = o[:128]
        out_ref[g * 128 : (g + 1) * 128, D:] = o[128:]
        lse = jnp.where(some, base * SCALE + jnp.log(safe), NEG)
        eye = lax.broadcasted_iota(jnp.int32, (128, 128), 0) == lax.broadcasted_iota(jnp.int32, (128, 128), 1)
        for h in range(2):
            flat = jnp.sum(jnp.where(eye, lse[h * 128 : (h + 1) * 128], 0.0), axis=0, keepdims=True)
            lses[h : h + 1, g * 128 : (g + 1) * 128] = flat

    tops = [score(g) for g in range(2)]
    sums = [weigh(g, tops[g]) for g in range(2)]
    for g in range(2):
        gather(g, *sums[g])

    lse = jnp.concatenate([lses[0:1, :], lses[1:2, :]], axis=1)
    high = lse.astype(jnp.bfloat16).astype(jnp.float32)
    mid = (lse - high).astype(jnp.bfloat16).astype(jnp.float32)
    low = lse - high - mid
    row = lax.broadcasted_iota(jnp.int32, (16, 2 * D), 0)
    parts = jnp.where(row == 0, high, jnp.where(row == 1, mid, jnp.where(row == 2, low, 0.0)))
    out_ref[256:, :] = parts.astype(jnp.bfloat16)


def attend(steps, order, q, chunks):
    return pl.pallas_call(
        functools.partial(attend_kernel, steps),
        out_shape=[jax.ShapeDtypeStruct((ROWS, 2 * D), jnp.bfloat16)] * len(steps),
        in_specs=[pl.BlockSpec(memory_space=pltpu.SMEM)]
        + [pl.BlockSpec(memory_space=pltpu.VMEM)] * 17,
        out_specs=[pl.BlockSpec(memory_space=pltpu.VMEM)] * len(steps),
        scratch_shapes=[
            pltpu.VMEM((2, 256, 2048), jnp.float32),
            pltpu.VMEM((2, 256, 2048), jnp.bfloat16),
            pltpu.VMEM((32, 2048), jnp.float32),
            pltpu.VMEM((8, 256), jnp.float32),
        ],
        compiler_params=pltpu.CompilerParams(vmem_limit_bytes=24 << 20),
        cost_estimate=pl.CostEstimate(
            flops=len(steps) * 4 * 512 * 2048 * D,
            bytes_accessed=3 << 20,
            transcendentals=len(steps) * 512 * 2048,
        ),
        name="attend",
    )(order, q, *chunks)


def combine_kernel(*refs):
    part_refs, out_ref, lse_ref = refs[:4], refs[4], refs[5]
    lses = []
    for r in part_refs:
        x = r[256:, :].astype(jnp.float32)
        lses.append(x[0:1] + x[1:2] + x[2:3])
    top = functools.reduce(jnp.maximum, lses)
    ws = [jnp.exp(x - top) for x in lses]
    total = functools.reduce(jnp.add, ws)
    lse = top + jnp.log(total)
    ws = [w / total for w in ws]
    lse_ref[0:1, :] = lse[:, :256]
    lse_ref[1:2, :] = lse[:, 256:]
    lse_ref[2:8, :] = jnp.zeros((6, 256), jnp.float32)
    eye = lax.broadcasted_iota(jnp.int32, (128, 128), 0) == lax.broadcasted_iota(jnp.int32, (128, 128), 1)
    for h in range(2):
        for g in range(2):
            at = h * 256 + g * 128
            o = jnp.zeros((128, D), jnp.float32)
            for w, r in zip(ws, part_refs):
                column = jnp.sum(jnp.where(eye, w[:, at : at + 128], 0.0), axis=1, keepdims=True)
                o = o + column * r[g * 128 : (g + 1) * 128, h * D : (h + 1) * D].astype(jnp.float32)
            out_ref[g * 128 : (g + 1) * 128, h * D : (h + 1) * D] = o.astype(jnp.bfloat16)


def combine(parts):
    return pl.pallas_call(
        combine_kernel,
        out_shape=[
            jax.ShapeDtypeStruct((256, 2 * D), jnp.bfloat16),
            jax.ShapeDtypeStruct((8, 256), jnp.float32),
        ],
        in_specs=[pl.BlockSpec(memory_space=pltpu.VMEM)] * 4,
        out_specs=[pl.BlockSpec(memory_space=pltpu.VMEM)] * 2,
        compiler_params=pltpu.CompilerParams(vmem_limit_bytes=8 << 20),
        cost_estimate=pl.CostEstimate(flops=1 << 22, bytes_accessed=2 << 20, transcendentals=4096),
        name="combine",
    )(*parts)


def local(queries, keys, values, block_order):
    xh = lax.axis_index("xh")
    halves = jnp.stack([queries[:, : 2 * D], queries[:, 2 * D :]])
    to_send = jnp.broadcast_to(halves[None], (NY, 2, 128, 2 * D)).reshape(2 * NY, 128, 2 * D)
    q = lax.all_to_all(to_send, ("y", "xh"), split_axis=0, concat_axis=0, tiled=True)

    def half(which):
        return jnp.concatenate(
            [lax.dynamic_slice_in_dim(a, which * D, D, 1) for a in (keys, values)], axis=1
        )

    mine, theirs = half(xh), half(1 - xh)
    chunks = [mine, cross(theirs, 0)]
    a_up, a_down = shift_z(mine, 1), shift_z(mine, -1)
    b_up, b_down = cross(theirs, 1), cross(theirs, -1)
    chunks += [a_up, a_down, b_up, b_down]
    for _ in range(2):
        a_up, a_down = shift_z(a_up, 1), shift_z(a_down, -1)
        b_up, b_down = shift_z(b_up, 1), shift_z(b_down, -1)
        chunks += [a_up, a_down, b_up, b_down]
    chunks += [shift_z(a_up, 1), shift_z(b_down, -1)]

    parts = []
    for steps in SPLIT:
        for step, part in zip(steps, attend(steps, block_order, q, chunks)):
            parts.append(shift_y(part, step) if step else part)
    out, lse = combine(parts)

    recv = lax.all_to_all(
        out.reshape(8, 32, 2 * D), ("xh", "xl", "c"), split_axis=0, concat_axis=0, tiled=True
    )
    attn = recv.reshape(2, 4, 32, 2 * D).transpose(2, 1, 0, 3).reshape(32, 16 * D)

    lse = lse[:2].reshape(2, 2, 128)
    own = lax.dynamic_index_in_dim(lse, xh, 1, keepdims=False)
    give = lax.dynamic_index_in_dim(lse, 1 - xh, 1, keepdims=False)
    take = lax.ppermute(give, "xh", [(0, 1), (1, 0)])
    first = jnp.where(xh == 0, own, take)
    last = jnp.where(xh == 0, take, own)
    return attn, jnp.concatenate([first, last], axis=0)


def solution(mesh):
    fine = Mesh(mesh.devices.reshape(NZ, NY, 2, 2, 2), ("z", "y", "xh", "xl", "c"))
    seq, head = ("z", "y", "xh"), ("xl", "c")
    in_specs = (P(seq, head), P(seq, head), P(seq, head), P())
    out_specs = (P(seq + head, None), P(head, seq))
    return jax.shard_map(local, mesh=fine, in_specs=in_specs, out_specs=out_specs, check_vma=False)
```

```python
import functools

import jax
import jax.numpy as jnp
from jax import lax
from jax.experimental import pallas as pl
from jax.experimental.pallas import tpu as pltpu
from jax.sharding import Mesh
from jax.sharding import PartitionSpec as P


D = 256
BLK = 64
NZ, NY = 8, 4
SCALE = D**-0.5
LOG2E = 1.4426950408889634
NEG = -1e30
ROWS = 136

CHUNKS = [(0, 0), (0, 1)]
for _k in (1, 2, 3):
    CHUNKS += [(-_k, 0), (_k, 0), (-_k, 1), (_k, 1)]
CHUNKS += [(4, 0), (4, 1)]
OWNERS = ((2, 1), (2, 0), (1, 1), (3, 1), (1, 0), (3, 0), (0, 1), (0, 0))


def shift_z(x, step):
    return lax.ppermute(x, "z", [(i, (i + step) % NZ) for i in range(NZ)])


def cross(x, step):
    pairs = [
        (z * 2 + h, ((z + step) % NZ) * 2 + 1 - h) for z in range(NZ) for h in range(2)
    ]
    return lax.ppermute(x, ("z", "xh"), pairs)


def spread_kernel(q_hbm, k_hbm, v_hbm, mine_ref, theirs_ref, send_ref, q_ref, k_ref, v_ref, sems):
    pairs = ((k_hbm, k_ref), (v_hbm, v_ref), (q_hbm, q_ref))
    copies = [pltpu.make_async_copy(a, b, sems.at[i]) for i, (a, b) in enumerate(pairs)]
    for copy in copies:
        copy.start()
    copies[0].wait()
    copies[1].wait()
    xh = lax.axis_index("xh")
    for out_ref, which in ((mine_ref, xh), (theirs_ref, 1 - xh)):
        at = pl.multiple_of(which * D, D)
        out_ref[:, :D] = k_ref[:, pl.ds(at, D)]
        out_ref[:, D:] = v_ref[:, pl.ds(at, D)]
    copies[2].wait()
    for h in range(2):
        x = q_ref[:, h * 2 * D : (h + 1) * 2 * D]
        for y in range(NY):
            send_ref[2 * y + h] = x


def spread(queries, keys, values):
    half = jax.ShapeDtypeStruct((128, 2 * D), jnp.bfloat16)
    return pl.pallas_call(
        spread_kernel,
        out_shape=[half, half, jax.ShapeDtypeStruct((2 * NY, 128, 2 * D), jnp.bfloat16)],
        in_specs=[pl.BlockSpec(memory_space=pl.ANY)] * 3,
        out_specs=[pl.BlockSpec(memory_space=pltpu.VMEM)] * 3,
        scratch_shapes=[
            pltpu.VMEM((128, 4 * D), jnp.bfloat16),
            pltpu.VMEM((128, 2 * D), jnp.bfloat16),
            pltpu.VMEM((128, 2 * D), jnp.bfloat16),
            pltpu.SemaphoreType.DMA((3,)),
        ],
        compiler_params=pltpu.CompilerParams(vmem_limit_bytes=60 << 20),
        name="spread",
    )(queries, keys, values)


def attend_kernel(order_ref, q_ref, *refs):
    kv_refs, out_ref = refs[:16], refs[16]
    scores, weights, bias, values = refs[17:]
    z, y, xh = lax.axis_index("z"), lax.axis_index("y"), lax.axis_index("xh")
    columns = []
    for dz, other in CHUNKS:
        zz = lax.rem(z + (dz + NZ), NZ)
        block = ((zz * NY + y) * 2 + (1 - xh if other else xh)) * 2
        lane = lax.broadcasted_iota(jnp.int32, (8, 128), 1)
        columns.append(jnp.where(lane < BLK, order_ref[block], order_ref[block + 1]))
    owners = [lax.rem(y + step, NY) * 2 + (1 - xh if flip else xh) for step, flip in OWNERS]
    row_pos = [[order_ref[(z * NY * 2 + owner) * 2 + b] for b in range(2)] for owner in owners]
    count = len(owners) // 2
    keys = [jnp.concatenate([kv_refs[2 * p][:, :D], kv_refs[2 * p + 1][:, :D]], axis=0) for p in range(8)]
    for p in range(16):
        values[p * 128 : (p + 1) * 128, :] = kv_refs[p][:, D:]

    def start(n):
        q = []
        for g in range(2):
            x = q_ref[owners[2 * n + g]]
            q += [x[:, :D], x[:, D:]]
            for b in range(2):
                at = 8 * (4 * (n % 2) + 2 * g + b)
                for j in range(16):
                    bias[at : at + 8, j * 128 : (j + 1) * 128] = jnp.where(
                        columns[j] <= row_pos[2 * n + g][b], 0.0, NEG
                    )
        return jnp.concatenate(q, axis=0)

    def score(n, p, q):
        slot = n % 2
        s = lax.dot_general(q, keys[p], (((1,), (1,)), ((), ())), preferred_element_type=jnp.float32)
        for r in range(8):
            g, b = r // 4, r % 2
            part = s[r * BLK : (r + 1) * BLK]
            if OWNERS[2 * n + g][0] == 0 and p == 0:
                at = row_pos[2 * n + g][b] * BLK + lax.broadcasted_iota(jnp.int32, (BLK, 1), 0)
                lane = lax.broadcasted_iota(jnp.int32, (1, 128), 1)
                cols = [columns[j][:1] * BLK + lane % BLK for j in range(2)]
                part = jnp.where(jnp.concatenate(cols, axis=1) <= at, part, NEG)
            else:
                at = 8 * (4 * slot + 2 * g + b)
                part = part + bias[at : at + 1, p * D : (p + 1) * D]
            scores[slot, r * BLK : (r + 1) * BLK, p * D : (p + 1) * D] = part

    def weigh(n, i):
        slot, rows = n % 2, slice(16 * i, 16 * i + 16)
        s = scores[slot, rows, :]
        top = jnp.max(s, axis=1, keepdims=True)
        base = jnp.where(top > 0.5 * NEG, top, 0.0)
        w = jnp.exp2((s - base) * (SCALE * LOG2E))
        weights[slot, rows, :] = w.astype(jnp.bfloat16)
        return base, jnp.sum(w, axis=1, keepdims=True)

    def finish(n, stats):
        acc = jnp.dot(weights[n % 2], values[...], preferred_element_type=jnp.float32)
        base = jnp.concatenate([x for x, _ in stats], axis=0)
        total = jnp.concatenate([x for _, x in stats], axis=0)
        some = total > 0.0
        safe = jnp.where(some, total, 1.0)
        o = (acc / safe).astype(jnp.bfloat16)
        lse = jnp.where(some, base * SCALE + jnp.log(safe), NEG)
        eye = lax.broadcasted_iota(jnp.int32, (128, 128), 0) == lax.broadcasted_iota(jnp.int32, (128, 128), 1)
        row = lax.broadcasted_iota(jnp.int32, (8, 128), 0)
        for g in range(2):
            owner = owners[2 * n + g]
            tail = jnp.zeros((8, 128), jnp.float32)
            for h in range(2):
                at = (2 * g + h) * 128
                flat = jnp.sum(jnp.where(eye, lse[at : at + 128], 0.0), axis=0, keepdims=True)
                high = flat.astype(jnp.bfloat16).astype(jnp.float32)
                mid = (flat - high).astype(jnp.bfloat16).astype(jnp.float32)
                for i, part in enumerate((high, mid, flat - high - mid)):
                    tail = jnp.where(row == 3 * h + i, part, tail)
            tail = tail.astype(jnp.bfloat16)
            for j in range(4):
                for h in range(2):
                    at = (2 * g + h) * 128 + j * 32
                    for i in range(2):
                        to = (2 * h + i) * 32
                        out_ref[owner * 4 + j, to : to + 32, :] = o[at : at + 32, i * 128 : (i + 1) * 128]
                out_ref[owner * 4 + j, 128:, :] = tail

    q = start(0)
    for p in range(8):
        score(0, p, q)
    for n in range(count):
        stats = []
        if n + 1 < count:
            q = start(n + 1)
        for p in range(8):
            if n + 1 < count:
                score(n + 1, p, q)
            stats += [weigh(n, 4 * p + i) for i in range(4)]
        finish(n, stats)


def attend(order, q, chunks):
    return pl.pallas_call(
        attend_kernel,
        out_shape=jax.ShapeDtypeStruct((32, ROWS, 128), jnp.bfloat16),
        in_specs=[pl.BlockSpec(memory_space=pltpu.SMEM)]
        + [pl.BlockSpec(memory_space=pltpu.VMEM)] * 17,
        out_specs=pl.BlockSpec(memory_space=pltpu.VMEM),
        scratch_shapes=[
            pltpu.VMEM((2, 512, 2048), jnp.float32),
            pltpu.VMEM((2, 512, 2048), jnp.bfloat16),
            pltpu.VMEM((64, 2048), jnp.float32),
            pltpu.VMEM((2048, D), jnp.bfloat16),
        ],
        compiler_params=pltpu.CompilerParams(vmem_limit_bytes=32 << 20),
        cost_estimate=pl.CostEstimate(
            flops=len(OWNERS) * 4 * 256 * 2048 * D,
            bytes_accessed=3 << 20,
            transcendentals=len(OWNERS) * 256 * 2048,
        ),
        name="attend",
    )(order, q, *chunks)


def combine_kernel(recv_ref, out_ref, lse_ref):
    mine = lax.axis_index("xl") * 2 + lax.axis_index("c")

    def parts_of(n):
        x = recv_ref[n, 128:, :].astype(jnp.float32)
        return [x[3 * h : 3 * h + 1] + x[3 * h + 1 : 3 * h + 2] + x[3 * h + 2 : 3 * h + 3] for h in range(2)]

    def merge(lses):
        top = functools.reduce(jnp.maximum, lses)
        ws = [jnp.exp(x - top) for x in lses]
        return top, ws, functools.reduce(jnp.add, ws)

    lane = lax.broadcasted_iota(jnp.int32, (32, 128), 1)
    pick = lane == lax.broadcasted_iota(jnp.int32, (32, 128), 0) + mine * 32
    for xh in range(2):
        for group in range(4):
            sources = [(y * 2 + xh) * 4 + group for y in range(NY)]
            lses = [parts_of(n) for n in sources]
            for h in range(2):
                _, ws, total = merge([x[h] for x in lses])
                columns = [jnp.sum(jnp.where(pick, w / total, 0.0), axis=1, keepdims=True) for w in ws]
                for i in range(2):
                    at = (2 * h + i) * 32
                    o = functools.reduce(
                        jnp.add,
                        [c * recv_ref[n, at : at + 32, :].astype(jnp.float32) for c, n in zip(columns, sources)],
                    )
                    col = group * 4 * D + xh * 2 * D + h * D + i * 128
                    out_ref[:, col : col + 128] = o.astype(jnp.bfloat16)
        lses = [parts_of((y * 2 + xh) * 4 + mine) for y in range(NY)]
        for h in range(2):
            top, _, total = merge([x[h] for x in lses])
            lse_ref[2 * xh + h : 2 * xh + h + 1, :] = top + jnp.log(total)


def combine(recv):
    return pl.pallas_call(
        combine_kernel,
        out_shape=[
            jax.ShapeDtypeStruct((32, 16 * D), jnp.bfloat16),
            jax.ShapeDtypeStruct((4, 128), jnp.float32),
        ],
        in_specs=[pl.BlockSpec(memory_space=pltpu.VMEM)],
        out_specs=[pl.BlockSpec(memory_space=pltpu.VMEM)] * 2,
        compiler_params=pltpu.CompilerParams(vmem_limit_bytes=8 << 20),
        cost_estimate=pl.CostEstimate(flops=1 << 22, bytes_accessed=2 << 20, transcendentals=4096),
        name="combine",
    )(recv)


def local(queries, keys, values, block_order):
    mine, theirs, to_send = spread(queries, keys, values)
    q = lax.all_to_all(to_send, ("y", "xh"), split_axis=0, concat_axis=0, tiled=True)

    chunks = [mine, cross(theirs, 0)]
    a_up, a_down = shift_z(mine, 1), shift_z(mine, -1)
    b_up, b_down = cross(theirs, 1), cross(theirs, -1)
    chunks += [a_up, a_down, b_up, b_down]
    for _ in range(2):
        a_up, a_down = shift_z(a_up, 1), shift_z(a_down, -1)
        b_up, b_down = shift_z(b_up, 1), shift_z(b_down, -1)
        chunks += [a_up, a_down, b_up, b_down]
    chunks += [shift_z(a_up, 1), shift_z(b_down, -1)]

    pieces = attend(block_order, q, chunks)
    recv = lax.all_to_all(pieces, ("y", "xh", "xl", "c"), split_axis=0, concat_axis=0, tiled=True)
    return combine(recv)


def solution(mesh):
    fine = Mesh(mesh.devices.reshape(NZ, NY, 2, 2, 2), ("z", "y", "xh", "xl", "c"))
    seq, head = ("z", "y", "xh"), ("xl", "c")
    in_specs = (P(seq, head), P(seq, head), P(seq, head), P())
    out_specs = (P(seq + head, None), P(head, seq))
    return jax.shard_map(local, mesh=fine, in_specs=in_specs, out_specs=out_specs, check_vma=False)
```

```python
import functools

import jax
import jax.numpy as jnp
from jax import lax
from jax.experimental import pallas as pl
from jax.experimental.pallas import tpu as pltpu
from jax.sharding import Mesh
from jax.sharding import PartitionSpec as P


D = 256
BLK = 64
NZ, NY = 8, 4
SCALE = D**-0.5
LOG2E = 1.4426950408889634
NEG = -1e30
ROWS = 136

CHUNKS = [(0, 0), (0, 1)]
for _k in (1, 2, 3):
    CHUNKS += [(-_k, 0), (_k, 0), (-_k, 1), (_k, 1)]
CHUNKS += [(4, 0), (4, 1)]
OWNERS = ((2, 1), (2, 0), (1, 1), (3, 1), (1, 0), (3, 0), (0, 1), (0, 0))


def shift_z(x, step):
    return lax.ppermute(x, "z", [(i, (i + step) % NZ) for i in range(NZ)])


def from_y(x, step):
    return lax.ppermute(x, "y", [((i + step) % NY, i) for i in range(NY)])


def cross(x, step):
    pairs = [
        (z * 2 + h, ((z + step) % NZ) * 2 + 1 - h) for z in range(NZ) for h in range(2)
    ]
    return lax.ppermute(x, ("z", "xh"), pairs)


def spread_kernel(q_hbm, k_hbm, v_hbm, all_ref, theirs_ref, mine_ref, q_ref, k_ref, v_ref, sems):
    pairs = ((k_hbm, k_ref), (v_hbm, v_ref), (q_hbm, q_ref))
    copies = [pltpu.make_async_copy(a, b, sems.at[i]) for i, (a, b) in enumerate(pairs)]
    for copy in copies:
        copy.start()
    for copy in copies:
        copy.wait()
    xh = lax.axis_index("xh")
    own, other = pl.multiple_of(xh * D, D), pl.multiple_of((1 - xh) * D, D)
    mine_ref[:, :D] = k_ref[:, pl.ds(own, D)]
    mine_ref[:, D:] = v_ref[:, pl.ds(own, D)]
    for out_ref in (all_ref, theirs_ref):
        out_ref[:, :D] = k_ref[:, pl.ds(other, D)]
        out_ref[:, D : 2 * D] = v_ref[:, pl.ds(other, D)]
    all_ref[:, 2 * D :] = q_ref[:, pl.ds(pl.multiple_of((1 - xh) * 2 * D, 2 * D), 2 * D)]


def spread(queries, keys, values):
    half = jax.ShapeDtypeStruct((128, 2 * D), jnp.bfloat16)
    return pl.pallas_call(
        spread_kernel,
        out_shape=[jax.ShapeDtypeStruct((128, 4 * D), jnp.bfloat16), half, half],
        in_specs=[pl.BlockSpec(memory_space=pl.ANY)] * 3,
        out_specs=[pl.BlockSpec(memory_space=pltpu.VMEM)] * 3,
        scratch_shapes=[
            pltpu.VMEM((128, 4 * D), jnp.bfloat16),
            pltpu.VMEM((128, 2 * D), jnp.bfloat16),
            pltpu.VMEM((128, 2 * D), jnp.bfloat16),
            pltpu.SemaphoreType.DMA((3,)),
        ],
        compiler_params=pltpu.CompilerParams(vmem_limit_bytes=60 << 20),
        name="spread",
    )(queries, keys, values)


def join_rows_kernel(q_ref, side_ref, out_ref):
    xh = lax.axis_index("xh")
    out_ref[:128, :] = q_ref[:, pl.ds(pl.multiple_of(xh * 2 * D, 2 * D), 2 * D)]
    out_ref[128:, :] = side_ref[:, 2 * D :]


def join(kernel, count, *args):
    return pl.pallas_call(
        kernel,
        out_shape=[jax.ShapeDtypeStruct((256, 2 * D), jnp.bfloat16)] * count,
        in_specs=[pl.BlockSpec(memory_space=pltpu.VMEM)] * len(args),
        out_specs=[pl.BlockSpec(memory_space=pltpu.VMEM)] * count,
        compiler_params=pltpu.CompilerParams(vmem_limit_bytes=4 << 20),
        name="join",
    )(*args)


def attend_kernel(order_ref, *refs):
    q_refs, (k_ref, v_ref), kv_refs, out_ref = refs[:4], refs[4:6], refs[6:21], refs[21]
    scores, weights, bias, values = refs[22:]
    z, y, xh = lax.axis_index("z"), lax.axis_index("y"), lax.axis_index("xh")
    columns = []
    for dz, other in CHUNKS:
        zz = lax.rem(z + (dz + NZ), NZ)
        block = ((zz * NY + y) * 2 + (1 - xh if other else xh)) * 2
        lane = lax.broadcasted_iota(jnp.int32, (8, 128), 1)
        columns.append(jnp.where(lane < BLK, order_ref[block], order_ref[block + 1]))
    owners = [lax.rem(y + step, NY) * 2 + (1 - xh if flip else xh) for step, flip in OWNERS]
    row_pos = [[order_ref[(z * NY * 2 + owner) * 2 + b] for b in range(2)] for owner in owners]
    count = len(owners) // 2
    own = pl.ds(pl.multiple_of(xh * D, D), D)
    keys = [k_ref[:, own]] + [r[:, :D] for r in kv_refs]
    keys = [jnp.concatenate(keys[2 * p : 2 * p + 2], axis=0) for p in range(8)]
    values[:128, :] = v_ref[:, own]
    for p, r in enumerate(kv_refs):
        values[(p + 1) * 128 : (p + 2) * 128, :] = r[:, D : 2 * D]

    def start(n):
        q = []
        for g in range(2):
            step, flip = OWNERS[2 * n + g]
            x = q_refs[step][flip * 128 : (flip + 1) * 128, :]
            q += [x[:, :D], x[:, D:]]
            for b in range(2):
                at = 8 * (4 * (n % 2) + 2 * g + b)
                for j in range(16):
                    bias[at : at + 8, j * 128 : (j + 1) * 128] = jnp.where(
                        columns[j] <= row_pos[2 * n + g][b], 0.0, NEG
                    )
        return jnp.concatenate(q, axis=0)

    def score(n, p, q):
        slot = n % 2
        s = lax.dot_general(q, keys[p], (((1,), (1,)), ((), ())), preferred_element_type=jnp.float32)
        for r in range(8):
            g, b = r // 4, r % 2
            part = s[r * BLK : (r + 1) * BLK]
            if OWNERS[2 * n + g][0] == 0 and p == 0:
                at = row_pos[2 * n + g][b] * BLK + lax.broadcasted_iota(jnp.int32, (BLK, 1), 0)
                lane = lax.broadcasted_iota(jnp.int32, (1, 128), 1)
                cols = [columns[j][:1] * BLK + lane % BLK for j in range(2)]
                part = jnp.where(jnp.concatenate(cols, axis=1) <= at, part, NEG)
            else:
                at = 8 * (4 * slot + 2 * g + b)
                part = part + bias[at : at + 1, p * D : (p + 1) * D]
            scores[slot, r * BLK : (r + 1) * BLK, p * D : (p + 1) * D] = part

    def weigh(n, i):
        slot, rows = n % 2, slice(16 * i, 16 * i + 16)
        s = scores[slot, rows, :]
        top = jnp.max(s, axis=1, keepdims=True)
        base = jnp.where(top > 0.5 * NEG, top, 0.0)
        w = jnp.exp2((s - base) * (SCALE * LOG2E))
        weights[slot, rows, :] = w.astype(jnp.bfloat16)
        return base, jnp.sum(w, axis=1, keepdims=True)

    def finish(n, stats):
        acc = jnp.dot(weights[n % 2], values[...], preferred_element_type=jnp.float32)
        base = jnp.concatenate([x for x, _ in stats], axis=0)
        total = jnp.concatenate([x for _, x in stats], axis=0)
        o = (acc * jnp.where(total > 0.0, 1.0 / total, 0.0)).astype(jnp.bfloat16)
        eye = lax.broadcasted_iota(jnp.int32, (128, 128), 0) == lax.broadcasted_iota(jnp.int32, (128, 128), 1)
        row = lax.broadcasted_iota(jnp.int32, (8, 128), 0)
        for g in range(2):
            owner = owners[2 * n + g]
            tail = jnp.zeros((8, 128), jnp.float32)
            for h in range(2):
                at = (2 * g + h) * 128
                top, sums = (
                    jnp.sum(jnp.where(eye, x[at : at + 128], 0.0), axis=0, keepdims=True)
                    for x in (base, total)
                )
                flat = jnp.where(sums > 0.0, top * SCALE + jnp.log(sums), NEG)
                high = flat.astype(jnp.bfloat16).astype(jnp.float32)
                mid = (flat - high).astype(jnp.bfloat16).astype(jnp.float32)
                for i, part in enumerate((high, mid, flat - high - mid)):
                    tail = jnp.where(row == 3 * h + i, part, tail)
            tail = tail.astype(jnp.bfloat16)
            for j in range(4):
                for h in range(2):
                    at = (2 * g + h) * 128 + j * 32
                    for i in range(2):
                        to = (2 * h + i) * 32
                        out_ref[owner * 4 + j, to : to + 32, :] = o[at : at + 32, i * 128 : (i + 1) * 128]
                out_ref[owner * 4 + j, 128:, :] = tail

    q = start(0)
    for p in range(8):
        score(0, p, q)
    for n in range(count):
        stats = []
        if n + 1 < count:
            q = start(n + 1)
        for p in range(8):
            if n + 1 < count:
                score(n + 1, p, q)
            stats += [weigh(n, 4 * p + i) for i in range(4)]
        finish(n, stats)


def attend(order, queries, keys, values, chunks):
    return pl.pallas_call(
        attend_kernel,
        out_shape=jax.ShapeDtypeStruct((32, ROWS, 128), jnp.bfloat16),
        in_specs=[pl.BlockSpec(memory_space=pltpu.SMEM)]
        + [pl.BlockSpec(memory_space=pltpu.VMEM)] * 21,
        out_specs=pl.BlockSpec(memory_space=pltpu.VMEM),
        scratch_shapes=[
            pltpu.VMEM((2, 512, 2048), jnp.float32),
            pltpu.VMEM((2, 512, 2048), jnp.bfloat16),
            pltpu.VMEM((64, 2048), jnp.float32),
            pltpu.VMEM((2048, D), jnp.bfloat16),
        ],
        compiler_params=pltpu.CompilerParams(vmem_limit_bytes=32 << 20),
        cost_estimate=pl.CostEstimate(
            flops=len(OWNERS) * 4 * 256 * 2048 * D,
            bytes_accessed=3 << 20,
            transcendentals=len(OWNERS) * 256 * 2048,
        ),
        name="attend",
    )(order, *queries, keys, values, *chunks)


def combine_kernel(recv_ref, out_ref, lse_ref):
    mine = lax.axis_index("xl") * 2 + lax.axis_index("c")

    def parts_of(n):
        x = recv_ref[n, 128:, :].astype(jnp.float32)
        return [x[3 * h : 3 * h + 1] + x[3 * h + 1 : 3 * h + 2] + x[3 * h + 2 : 3 * h + 3] for h in range(2)]

    def merge(lses):
        top = functools.reduce(jnp.maximum, lses)
        ws = [jnp.exp(x - top) for x in lses]
        return top, ws, functools.reduce(jnp.add, ws)

    lane = lax.broadcasted_iota(jnp.int32, (32, 128), 1)
    pick = lane == lax.broadcasted_iota(jnp.int32, (32, 128), 0) + mine * 32
    for xh in range(2):
        for group in range(4):
            sources = [(y * 2 + xh) * 4 + group for y in range(NY)]
            lses = [parts_of(n) for n in sources]
            for h in range(2):
                _, ws, total = merge([x[h] for x in lses])
                columns = [jnp.sum(jnp.where(pick, w / total, 0.0), axis=1, keepdims=True) for w in ws]
                for i in range(2):
                    at = (2 * h + i) * 32
                    o = functools.reduce(
                        jnp.add,
                        [c * recv_ref[n, at : at + 32, :].astype(jnp.float32) for c, n in zip(columns, sources)],
                    )
                    col = group * 4 * D + xh * 2 * D + h * D + i * 128
                    out_ref[:, col : col + 128] = o.astype(jnp.bfloat16)
        lses = [parts_of((y * 2 + xh) * 4 + mine) for y in range(NY)]
        for h in range(2):
            top, _, total = merge([x[h] for x in lses])
            lse_ref[2 * xh + h : 2 * xh + h + 1, :] = top + jnp.log(total)


def combine(recv):
    return pl.pallas_call(
        combine_kernel,
        out_shape=[
            jax.ShapeDtypeStruct((32, 16 * D), jnp.bfloat16),
            jax.ShapeDtypeStruct((4, 128), jnp.float32),
        ],
        in_specs=[pl.BlockSpec(memory_space=pltpu.VMEM)],
        out_specs=[pl.BlockSpec(memory_space=pltpu.VMEM)] * 2,
        compiler_params=pltpu.CompilerParams(vmem_limit_bytes=8 << 20),
        cost_estimate=pl.CostEstimate(flops=1 << 22, bytes_accessed=2 << 20, transcendentals=4096),
        name="combine",
    )(recv)


def local(queries, keys, values, block_order):
    everything, theirs, mine = spread(queries, keys, values)
    side = cross(everything, 0)
    joined = join(join_rows_kernel, 1, queries, side)[0]
    q = [joined] + [from_y(joined, step) for step in (1, 2, 3)]

    chunks = [side]
    a_up, a_down = shift_z(mine, 1), shift_z(mine, -1)
    b_up, b_down = cross(theirs, 1), cross(theirs, -1)
    chunks += [a_up, a_down, b_up, b_down]
    for _ in range(2):
        a_up, a_down = shift_z(a_up, 1), shift_z(a_down, -1)
        b_up, b_down = shift_z(b_up, 1), shift_z(b_down, -1)
        chunks += [a_up, a_down, b_up, b_down]
    chunks += [shift_z(a_up, 1), shift_z(b_down, -1)]

    pieces = attend(block_order, q, keys, values, chunks)
    recv = lax.all_to_all(pieces, ("y", "xh", "xl", "c"), split_axis=0, concat_axis=0, tiled=True)
    return combine(recv)


def solution(mesh):
    fine = Mesh(mesh.devices.reshape(NZ, NY, 2, 2, 2), ("z", "y", "xh", "xl", "c"))
    seq, head = ("z", "y", "xh"), ("xl", "c")
    in_specs = (P(seq, head), P(seq, head), P(seq, head), P())
    out_specs = (P(seq + head, None), P(head, seq))
    return jax.shard_map(local, mesh=fine, in_specs=in_specs, out_specs=out_specs, check_vma=False)
```

```python
import functools

import jax
import jax.numpy as jnp
from jax import lax
from jax.experimental import pallas as pl
from jax.experimental.pallas import tpu as pltpu
from jax.sharding import Mesh
from jax.sharding import PartitionSpec as P


D = 256
BLK = 64
NZ, NY = 8, 4
SCALE = D**-0.5
LOG2E = 1.4426950408889634
NEG = -1e30
ROWS = 136

CHUNKS = [(0, 0), (0, 1)]
for _k in (1, 2, 3):
    CHUNKS += [(-_k, 0), (_k, 0), (-_k, 1), (_k, 1)]
CHUNKS += [(4, 0), (4, 1)]
OWNERS = ((2, 1), (2, 0), (1, 1), (3, 1), (1, 0), (3, 0), (0, 1), (0, 0))


def shift_z(x, step):
    return lax.ppermute(x, "z", [(i, (i + step) % NZ) for i in range(NZ)])


def from_y(x, step):
    return lax.ppermute(x, "y", [((i + step) % NY, i) for i in range(NY)])


def cross(x, step):
    pairs = [
        (z * 2 + h, ((z + step) % NZ) * 2 + 1 - h) for z in range(NZ) for h in range(2)
    ]
    return lax.ppermute(x, ("z", "xh"), pairs)


def spread_kernel(q_hbm, k_hbm, v_hbm, all_ref, theirs_ref, mine_ref, mineq_ref, q_ref, k_ref, v_ref, sems):
    pairs = ((k_hbm, k_ref), (v_hbm, v_ref), (q_hbm, q_ref))
    copies = [pltpu.make_async_copy(a, b, sems.at[i]) for i, (a, b) in enumerate(pairs)]
    for copy in copies:
        copy.start()
    for copy in copies:
        copy.wait()
    xh = lax.axis_index("xh")
    own, other = pl.multiple_of(xh * D, D), pl.multiple_of((1 - xh) * D, D)
    mine_ref[:, :D] = k_ref[:, pl.ds(own, D)]
    mine_ref[:, D:] = v_ref[:, pl.ds(own, D)]
    for out_ref in (all_ref, theirs_ref):
        out_ref[:, :D] = k_ref[:, pl.ds(other, D)]
        out_ref[:, D : 2 * D] = v_ref[:, pl.ds(other, D)]
    all_ref[:, 2 * D :] = q_ref[:, pl.ds(pl.multiple_of((1 - xh) * 2 * D, 2 * D), 2 * D)]
    mineq_ref[...] = q_ref[:, pl.ds(pl.multiple_of(xh * 2 * D, 2 * D), 2 * D)]


def spread(queries, keys, values):
    half = jax.ShapeDtypeStruct((128, 2 * D), jnp.bfloat16)
    return pl.pallas_call(
        spread_kernel,
        out_shape=[jax.ShapeDtypeStruct((128, 4 * D), jnp.bfloat16), half, half, half],
        in_specs=[pl.BlockSpec(memory_space=pl.ANY)] * 3,
        out_specs=[pl.BlockSpec(memory_space=pltpu.VMEM)] * 4,
        scratch_shapes=[
            pltpu.VMEM((128, 4 * D), jnp.bfloat16),
            pltpu.VMEM((128, 2 * D), jnp.bfloat16),
            pltpu.VMEM((128, 2 * D), jnp.bfloat16),
            pltpu.SemaphoreType.DMA((3,)),
        ],
        compiler_params=pltpu.CompilerParams(vmem_limit_bytes=54800 << 10),
        name="spread",
    )(queries, keys, values)


def join_rows_kernel(q_ref, side_ref, out_ref):
    out_ref[:128, :] = q_ref[...]
    out_ref[128:, :] = side_ref[:, 2 * D :]


def join(kernel, count, *args):
    return pl.pallas_call(
        kernel,
        out_shape=[jax.ShapeDtypeStruct((256, 2 * D), jnp.bfloat16)] * count,
        in_specs=[pl.BlockSpec(memory_space=pltpu.VMEM)] * len(args),
        out_specs=[pl.BlockSpec(memory_space=pltpu.VMEM)] * count,
        compiler_params=pltpu.CompilerParams(vmem_limit_bytes=4 << 20),
        name="join",
    )(*args)


def attend_kernel(order_ref, *refs):
    q_refs, (k_ref, v_ref), kv_refs, out_ref = refs[:4], refs[4:6], refs[6:21], refs[21]
    scores, weights, bias, values = refs[22:]
    z, y, xh = lax.axis_index("z"), lax.axis_index("y"), lax.axis_index("xh")
    columns = []
    for dz, other in CHUNKS:
        zz = lax.rem(z + (dz + NZ), NZ)
        block = ((zz * NY + y) * 2 + (1 - xh if other else xh)) * 2
        lane = lax.broadcasted_iota(jnp.int32, (8, 128), 1)
        columns.append(jnp.where(lane < BLK, order_ref[block], order_ref[block + 1]))
    owners = [lax.rem(y + step, NY) * 2 + (1 - xh if flip else xh) for step, flip in OWNERS]
    row_pos = [[order_ref[(z * NY * 2 + owner) * 2 + b] for b in range(2)] for owner in owners]
    count = len(owners) // 2
    own = pl.ds(pl.multiple_of(xh * D, D), D)
    keys = [k_ref[:, own]] + [r[:, :D] for r in kv_refs]
    keys = [jnp.concatenate(keys[2 * p : 2 * p + 2], axis=0) for p in range(8)]
    values[:128, :] = v_ref[:, own]
    for p, r in enumerate(kv_refs):
        values[(p + 1) * 128 : (p + 2) * 128, :] = r[:, D : 2 * D]

    def start(n):
        q = []
        for g in range(2):
            step, flip = OWNERS[2 * n + g]
            x = q_refs[step][flip * 128 : (flip + 1) * 128, :]
            q += [x[:, :D], x[:, D:]]
            for b in range(2):
                at = 8 * (4 * (n % 2) + 2 * g + b)
                for j in range(16):
                    bias[at : at + 8, j * 128 : (j + 1) * 128] = jnp.where(
                        columns[j] <= row_pos[2 * n + g][b], 0.0, NEG
                    )
        return jnp.concatenate(q, axis=0)

    def score(n, p, q):
        slot = n % 2
        s = lax.dot_general(q, keys[p], (((1,), (1,)), ((), ())), preferred_element_type=jnp.float32)
        for r in range(8):
            g, b = r // 4, r % 2
            part = s[r * BLK : (r + 1) * BLK]
            if OWNERS[2 * n + g][0] == 0 and p == 0:
                at = row_pos[2 * n + g][b] * BLK + lax.broadcasted_iota(jnp.int32, (BLK, 1), 0)
                lane = lax.broadcasted_iota(jnp.int32, (1, 128), 1)
                cols = [columns[j][:1] * BLK + lane % BLK for j in range(2)]
                part = jnp.where(jnp.concatenate(cols, axis=1) <= at, part, NEG)
            else:
                at = 8 * (4 * slot + 2 * g + b)
                part = part + bias[at : at + 1, p * D : (p + 1) * D]
            scores[slot, r * BLK : (r + 1) * BLK, p * D : (p + 1) * D] = part

    def weigh(n, i):
        slot, rows = n % 2, slice(16 * i, 16 * i + 16)
        s = scores[slot, rows, :]
        top = jnp.max(s, axis=1, keepdims=True)
        base = jnp.where(top > 0.5 * NEG, top, 0.0)
        w = jnp.exp2((s - base) * (SCALE * LOG2E))
        weights[slot, rows, :] = w.astype(jnp.bfloat16)
        return base, jnp.sum(w, axis=1, keepdims=True)

    def finish(n, stats):
        acc = jnp.dot(weights[n % 2], values[...], preferred_element_type=jnp.float32)
        base = jnp.concatenate([x for x, _ in stats], axis=0)
        total = jnp.concatenate([x for _, x in stats], axis=0)
        o = (acc * jnp.where(total > 0.0, 1.0 / total, 0.0)).astype(jnp.bfloat16)
        eye = lax.broadcasted_iota(jnp.int32, (128, 128), 0) == lax.broadcasted_iota(jnp.int32, (128, 128), 1)
        row = lax.broadcasted_iota(jnp.int32, (8, 128), 0)
        for g in range(2):
            owner = owners[2 * n + g]
            tail = jnp.zeros((8, 128), jnp.float32)
            for h in range(2):
                at = (2 * g + h) * 128
                top, sums = (
                    jnp.sum(jnp.where(eye, x[at : at + 128], 0.0), axis=0, keepdims=True)
                    for x in (base, total)
                )
                flat = jnp.where(sums > 0.0, top * SCALE + jnp.log(sums), NEG)
                high = flat.astype(jnp.bfloat16).astype(jnp.float32)
                mid = (flat - high).astype(jnp.bfloat16).astype(jnp.float32)
                for i, part in enumerate((high, mid, flat - high - mid)):
                    tail = jnp.where(row == 3 * h + i, part, tail)
            tail = tail.astype(jnp.bfloat16)
            for j in range(4):
                for h in range(2):
                    at = (2 * g + h) * 128 + j * 32
                    for i in range(2):
                        to = (2 * h + i) * 32
                        out_ref[owner * 4 + j, to : to + 32, :] = o[at : at + 32, i * 128 : (i + 1) * 128]
                out_ref[owner * 4 + j, 128:, :] = tail

    q = start(0)
    for p in range(8):
        score(0, p, q)
    for n in range(count):
        stats = []
        if n + 1 < count:
            q = start(n + 1)
        for p in range(8):
            if n + 1 < count:
                score(n + 1, p, q)
            stats += [weigh(n, 4 * p + i) for i in range(4)]
        finish(n, stats)


def attend(order, queries, keys, values, chunks):
    return pl.pallas_call(
        attend_kernel,
        out_shape=jax.ShapeDtypeStruct((32, ROWS, 128), jnp.bfloat16),
        in_specs=[pl.BlockSpec(memory_space=pltpu.SMEM)]
        + [pl.BlockSpec(memory_space=pltpu.VMEM)] * 21,
        out_specs=pl.BlockSpec(memory_space=pltpu.VMEM),
        scratch_shapes=[
            pltpu.VMEM((2, 512, 2048), jnp.float32),
            pltpu.VMEM((2, 512, 2048), jnp.bfloat16),
            pltpu.VMEM((64, 2048), jnp.float32),
            pltpu.VMEM((2048, D), jnp.bfloat16),
        ],
        compiler_params=pltpu.CompilerParams(vmem_limit_bytes=32 << 20),
        cost_estimate=pl.CostEstimate(
            flops=len(OWNERS) * 4 * 256 * 2048 * D,
            bytes_accessed=3 << 20,
            transcendentals=len(OWNERS) * 256 * 2048,
        ),
        name="attend",
    )(order, *queries, keys, values, *chunks)


def combine_kernel(recv_ref, out_ref, lse_ref):
    mine = lax.axis_index("xl") * 2 + lax.axis_index("c")

    def parts_of(n):
        x = recv_ref[n, 128:, :].astype(jnp.float32)
        return [x[3 * h : 3 * h + 1] + x[3 * h + 1 : 3 * h + 2] + x[3 * h + 2 : 3 * h + 3] for h in range(2)]

    def merge(lses):
        top = functools.reduce(jnp.maximum, lses)
        ws = [jnp.exp(x - top) for x in lses]
        return top, ws, functools.reduce(jnp.add, ws)

    lane = lax.broadcasted_iota(jnp.int32, (32, 128), 1)
    pick = lane == lax.broadcasted_iota(jnp.int32, (32, 128), 0) + mine * 32
    for xh in range(2):
        for group in range(4):
            sources = [(y * 2 + xh) * 4 + group for y in range(NY)]
            lses = [parts_of(n) for n in sources]
            for h in range(2):
                _, ws, total = merge([x[h] for x in lses])
                columns = [jnp.sum(jnp.where(pick, w / total, 0.0), axis=1, keepdims=True) for w in ws]
                for i in range(2):
                    at = (2 * h + i) * 32
                    o = functools.reduce(
                        jnp.add,
                        [c * recv_ref[n, at : at + 32, :].astype(jnp.float32) for c, n in zip(columns, sources)],
                    )
                    col = group * 4 * D + xh * 2 * D + h * D + i * 128
                    out_ref[:, col : col + 128] = o.astype(jnp.bfloat16)
        lses = [parts_of((y * 2 + xh) * 4 + mine) for y in range(NY)]
        for h in range(2):
            top, _, total = merge([x[h] for x in lses])
            lse_ref[2 * xh + h : 2 * xh + h + 1, :] = top + jnp.log(total)


def combine(recv):
    return pl.pallas_call(
        combine_kernel,
        out_shape=[
            jax.ShapeDtypeStruct((32, 16 * D), jnp.bfloat16),
            jax.ShapeDtypeStruct((4, 128), jnp.float32),
        ],
        in_specs=[pl.BlockSpec(memory_space=pltpu.VMEM)],
        out_specs=[pl.BlockSpec(memory_space=pltpu.VMEM)] * 2,
        compiler_params=pltpu.CompilerParams(vmem_limit_bytes=8 << 20),
        cost_estimate=pl.CostEstimate(flops=1 << 22, bytes_accessed=2 << 20, transcendentals=4096),
        name="combine",
    )(recv)


def local(queries, keys, values, block_order):
    everything, theirs, mine, mineq = spread(queries, keys, values)
    side = cross(everything, 0)
    joined = join(join_rows_kernel, 1, mineq, side)[0]
    q = [joined] + [from_y(joined, step) for step in (1, 2, 3)]

    chunks = [side]
    a_up, a_down = shift_z(mine, 1), shift_z(mine, -1)
    b_up, b_down = cross(theirs, 1), cross(theirs, -1)
    chunks += [a_up, a_down, b_up, b_down]
    for _ in range(2):
        a_up, a_down = shift_z(a_up, 1), shift_z(a_down, -1)
        b_up, b_down = shift_z(b_up, 1), shift_z(b_down, -1)
        chunks += [a_up, a_down, b_up, b_down]
    chunks += [shift_z(a_up, 1), shift_z(b_down, -1)]

    pieces = attend(block_order, q, keys, values, chunks)
    recv = lax.all_to_all(pieces, ("y", "xh", "xl", "c"), split_axis=0, concat_axis=0, tiled=True)
    return combine(recv)


def solution(mesh):
    fine = Mesh(mesh.devices.reshape(NZ, NY, 2, 2, 2), ("z", "y", "xh", "xl", "c"))
    seq, head = ("z", "y", "xh"), ("xl", "c")
    in_specs = (P(seq, head), P(seq, head), P(seq, head), P())
    out_specs = (P(seq + head, None), P(head, seq))
    return jax.shard_map(local, mesh=fine, in_specs=in_specs, out_specs=out_specs, check_vma=False)
```

```python
import functools

import jax
import jax.numpy as jnp
from jax import lax
from jax.experimental import pallas as pl
from jax.experimental.pallas import tpu as pltpu
from jax.sharding import Mesh
from jax.sharding import PartitionSpec as P


D = 256
BLK = 64
NZ, NY = 8, 4
SCALE = D**-0.5
LOG2E = 1.4426950408889634
NEG = -1e30
ROWS = 136

CHUNKS = [(0, 0), (0, 1)]
for _k in (1, 2, 3):
    CHUNKS += [(_k, 0), (-_k, 0), (_k, 1), (-_k, 1)]
CHUNKS += [(4, 0), (4, 1)]
OWNERS = ((2, 1), (2, 0), (1, 1), (3, 1), (1, 0), (3, 0), (0, 1), (0, 0))


def neighbour(z, side):
    if side == 0:
        return z
    if side == 1:
        return z ^ 1
    return (z + 1) % NZ if z % 2 else (z - 1) % NZ


def along(x, side):
    return lax.ppermute(x, "z", [(z, neighbour(z, side)) for z in range(NZ)])


def from_y(x, step):
    return lax.ppermute(x, "y", [((i + step) % NY, i) for i in range(NY)])


def cross(x, side):
    pairs = [(z * 2 + h, neighbour(z, side) * 2 + 1 - h) for z in range(NZ) for h in range(2)]
    return lax.ppermute(x, ("z", "xh"), pairs)


def spread_kernel(q_hbm, k_hbm, v_hbm, all_ref, theirs_ref, mine_ref, mineq_ref, q_ref, k_ref, v_ref, sems):
    pairs = ((k_hbm, k_ref), (v_hbm, v_ref), (q_hbm, q_ref))
    copies = [pltpu.make_async_copy(a, b, sems.at[i]) for i, (a, b) in enumerate(pairs)]
    for copy in copies:
        copy.start()
    for copy in copies:
        copy.wait()
    xh = lax.axis_index("xh")
    own, other = pl.multiple_of(xh * D, D), pl.multiple_of((1 - xh) * D, D)
    mine_ref[:, :D] = k_ref[:, pl.ds(own, D)]
    mine_ref[:, D:] = v_ref[:, pl.ds(own, D)]
    for out_ref in (all_ref, theirs_ref):
        out_ref[:, :D] = k_ref[:, pl.ds(other, D)]
        out_ref[:, D : 2 * D] = v_ref[:, pl.ds(other, D)]
    all_ref[:, 2 * D :] = q_ref[:, pl.ds(pl.multiple_of((1 - xh) * 2 * D, 2 * D), 2 * D)]
    mineq_ref[...] = q_ref[:, pl.ds(pl.multiple_of(xh * 2 * D, 2 * D), 2 * D)]


def spread(queries, keys, values):
    half = jax.ShapeDtypeStruct((128, 2 * D), jnp.bfloat16)
    return pl.pallas_call(
        spread_kernel,
        out_shape=[jax.ShapeDtypeStruct((128, 4 * D), jnp.bfloat16), half, half, half],
        in_specs=[pl.BlockSpec(memory_space=pl.ANY)] * 3,
        out_specs=[pl.BlockSpec(memory_space=pltpu.VMEM)] * 4,
        scratch_shapes=[
            pltpu.VMEM((128, 4 * D), jnp.bfloat16),
            pltpu.VMEM((128, 2 * D), jnp.bfloat16),
            pltpu.VMEM((128, 2 * D), jnp.bfloat16),
            pltpu.SemaphoreType.DMA((3,)),
        ],
        compiler_params=pltpu.CompilerParams(vmem_limit_bytes=54800 << 10),
        name="spread",
    )(queries, keys, values)


def join_rows_kernel(q_ref, side_ref, out_ref):
    out_ref[:128, :] = q_ref[...]
    out_ref[128:, :] = side_ref[:, 2 * D :]


def join(kernel, count, *args):
    return pl.pallas_call(
        kernel,
        out_shape=[jax.ShapeDtypeStruct((256, 2 * D), jnp.bfloat16)] * count,
        in_specs=[pl.BlockSpec(memory_space=pltpu.VMEM)] * len(args),
        out_specs=[pl.BlockSpec(memory_space=pltpu.VMEM)] * count,
        compiler_params=pltpu.CompilerParams(vmem_limit_bytes=4 << 20),
        name="join",
    )(*args)


def attend_kernel(order_ref, *refs):
    q_refs, (k_ref, v_ref), kv_refs, out_ref = refs[:4], refs[4:6], refs[6:21], refs[21]
    scores, weights, bias, values = refs[22:]
    z, y, xh = lax.axis_index("z"), lax.axis_index("y"), lax.axis_index("xh")
    columns = []
    for dz, other in CHUNKS:
        zz = lax.rem(z + (1 - 2 * lax.rem(z, 2)) * dz + NZ, NZ)
        block = ((zz * NY + y) * 2 + (1 - xh if other else xh)) * 2
        lane = lax.broadcasted_iota(jnp.int32, (8, 128), 1)
        columns.append(jnp.where(lane < BLK, order_ref[block], order_ref[block + 1]))
    owners = [lax.rem(y + step, NY) * 2 + (1 - xh if flip else xh) for step, flip in OWNERS]
    row_pos = [[order_ref[(z * NY * 2 + owner) * 2 + b] for b in range(2)] for owner in owners]
    count = len(owners) // 2
    own = pl.ds(pl.multiple_of(xh * D, D), D)
    keys = [k_ref[:, own]] + [r[:, :D] for r in kv_refs]
    keys = [jnp.concatenate(keys[2 * p : 2 * p + 2], axis=0) for p in range(8)]
    values[:128, :] = v_ref[:, own]
    for p, r in enumerate(kv_refs):
        values[(p + 1) * 128 : (p + 2) * 128, :] = r[:, D : 2 * D]

    def start(n):
        q = []
        for g in range(2):
            step, flip = OWNERS[2 * n + g]
            x = q_refs[step][flip * 128 : (flip + 1) * 128, :]
            q += [x[:, :D], x[:, D:]]
            for b in range(2):
                at = 8 * (4 * (n % 2) + 2 * g + b)
                for j in range(16):
                    bias[at : at + 8, j * 128 : (j + 1) * 128] = jnp.where(
                        columns[j] <= row_pos[2 * n + g][b], 0.0, NEG
                    )
        return jnp.concatenate(q, axis=0)

    def score(n, p, q):
        slot = n % 2
        s = lax.dot_general(q, keys[p], (((1,), (1,)), ((), ())), preferred_element_type=jnp.float32)
        for r in range(8):
            g, b = r // 4, r % 2
            part = s[r * BLK : (r + 1) * BLK]
            if OWNERS[2 * n + g][0] == 0 and p == 0:
                at = row_pos[2 * n + g][b] * BLK + lax.broadcasted_iota(jnp.int32, (BLK, 1), 0)
                lane = lax.broadcasted_iota(jnp.int32, (1, 128), 1)
                cols = [columns[j][:1] * BLK + lane % BLK for j in range(2)]
                part = jnp.where(jnp.concatenate(cols, axis=1) <= at, part, NEG)
            else:
                at = 8 * (4 * slot + 2 * g + b)
                part = part + bias[at : at + 1, p * D : (p + 1) * D]
            scores[slot, r * BLK : (r + 1) * BLK, p * D : (p + 1) * D] = part

    def weigh(n, i):
        slot, rows = n % 2, slice(16 * i, 16 * i + 16)
        s = scores[slot, rows, :]
        top = jnp.max(s, axis=1, keepdims=True)
        base = jnp.where(top > 0.5 * NEG, top, 0.0)
        w = jnp.exp2((s - base) * (SCALE * LOG2E))
        weights[slot, rows, :] = w.astype(jnp.bfloat16)
        return base, jnp.sum(w, axis=1, keepdims=True)

    def finish(n, stats):
        acc = jnp.dot(weights[n % 2], values[...], preferred_element_type=jnp.float32)
        base = jnp.concatenate([x for x, _ in stats], axis=0)
        total = jnp.concatenate([x for _, x in stats], axis=0)
        o = (acc * jnp.where(total > 0.0, 1.0 / total, 0.0)).astype(jnp.bfloat16)
        eye = lax.broadcasted_iota(jnp.int32, (128, 128), 0) == lax.broadcasted_iota(jnp.int32, (128, 128), 1)
        row = lax.broadcasted_iota(jnp.int32, (8, 128), 0)
        for g in range(2):
            owner = owners[2 * n + g]
            tail = jnp.zeros((8, 128), jnp.float32)
            for h in range(2):
                at = (2 * g + h) * 128
                top, sums = (
                    jnp.sum(jnp.where(eye, x[at : at + 128], 0.0), axis=0, keepdims=True)
                    for x in (base, total)
                )
                flat = jnp.where(sums > 0.0, top * SCALE + jnp.log(sums), NEG)
                high = flat.astype(jnp.bfloat16).astype(jnp.float32)
                mid = (flat - high).astype(jnp.bfloat16).astype(jnp.float32)
                for i, part in enumerate((high, mid, flat - high - mid)):
                    tail = jnp.where(row == 3 * h + i, part, tail)
            tail = tail.astype(jnp.bfloat16)
            for j in range(4):
                for h in range(2):
                    at = (2 * g + h) * 128 + j * 32
                    for i in range(2):
                        to = (2 * h + i) * 32
                        out_ref[owner * 4 + j, to : to + 32, :] = o[at : at + 32, i * 128 : (i + 1) * 128]
                out_ref[owner * 4 + j, 128:, :] = tail

    q = start(0)
    for p in range(8):
        score(0, p, q)
    for n in range(count):
        stats = []
        if n + 1 < count:
            q = start(n + 1)
        for p in range(8):
            if n + 1 < count:
                score(n + 1, p, q)
            stats += [weigh(n, 4 * p + i) for i in range(4)]
        finish(n, stats)


def attend(order, queries, keys, values, chunks):
    return pl.pallas_call(
        attend_kernel,
        out_shape=jax.ShapeDtypeStruct((32, ROWS, 128), jnp.bfloat16),
        in_specs=[pl.BlockSpec(memory_space=pltpu.SMEM)]
        + [pl.BlockSpec(memory_space=pltpu.VMEM)] * 21,
        out_specs=pl.BlockSpec(memory_space=pltpu.VMEM),
        scratch_shapes=[
            pltpu.VMEM((2, 512, 2048), jnp.float32),
            pltpu.VMEM((2, 512, 2048), jnp.bfloat16),
            pltpu.VMEM((64, 2048), jnp.float32),
            pltpu.VMEM((2048, D), jnp.bfloat16),
        ],
        compiler_params=pltpu.CompilerParams(vmem_limit_bytes=32 << 20),
        cost_estimate=pl.CostEstimate(
            flops=len(OWNERS) * 4 * 256 * 2048 * D,
            bytes_accessed=3 << 20,
            transcendentals=len(OWNERS) * 256 * 2048,
        ),
        name="attend",
    )(order, *queries, keys, values, *chunks)


def combine_kernel(recv_ref, out_ref, lse_ref):
    mine = lax.axis_index("xl") * 2 + lax.axis_index("c")

    def parts_of(n):
        x = recv_ref[n, 128:, :].astype(jnp.float32)
        return [x[3 * h : 3 * h + 1] + x[3 * h + 1 : 3 * h + 2] + x[3 * h + 2 : 3 * h + 3] for h in range(2)]

    def merge(lses):
        top = functools.reduce(jnp.maximum, lses)
        ws = [jnp.exp(x - top) for x in lses]
        return top, ws, functools.reduce(jnp.add, ws)

    lane = lax.broadcasted_iota(jnp.int32, (32, 128), 1)
    pick = lane == lax.broadcasted_iota(jnp.int32, (32, 128), 0) + mine * 32
    for xh in range(2):
        for group in range(4):
            sources = [(y * 2 + xh) * 4 + group for y in range(NY)]
            lses = [parts_of(n) for n in sources]
            for h in range(2):
                _, ws, total = merge([x[h] for x in lses])
                share = 1.0 / total
                columns = [jnp.sum(jnp.where(pick, w * share, 0.0), axis=1, keepdims=True) for w in ws]
                for i in range(2):
                    at = (2 * h + i) * 32
                    o = functools.reduce(
                        jnp.add,
                        [c * recv_ref[n, at : at + 32, :].astype(jnp.float32) for c, n in zip(columns, sources)],
                    )
                    col = group * 4 * D + xh * 2 * D + h * D + i * 128
                    out_ref[:, col : col + 128] = o.astype(jnp.bfloat16)
        lses = [parts_of((y * 2 + xh) * 4 + mine) for y in range(NY)]
        for h in range(2):
            top, _, total = merge([x[h] for x in lses])
            lse_ref[2 * xh + h : 2 * xh + h + 1, :] = top + jnp.log(total)


def combine(recv):
    return pl.pallas_call(
        combine_kernel,
        out_shape=[
            jax.ShapeDtypeStruct((32, 16 * D), jnp.bfloat16),
            jax.ShapeDtypeStruct((4, 128), jnp.float32),
        ],
        in_specs=[pl.BlockSpec(memory_space=pltpu.VMEM)],
        out_specs=[pl.BlockSpec(memory_space=pltpu.VMEM)] * 2,
        compiler_params=pltpu.CompilerParams(vmem_limit_bytes=8 << 20),
        cost_estimate=pl.CostEstimate(flops=1 << 22, bytes_accessed=2 << 20, transcendentals=4096),
        name="combine",
    )(recv)


def local(queries, keys, values, block_order):
    everything, theirs, mine, mineq = spread(queries, keys, values)
    side = cross(everything, 0)
    joined = join(join_rows_kernel, 1, mineq, side)[0]
    q = [joined] + [from_y(joined, step) for step in (1, 2, 3)]

    chunks = [side]
    a1, a2 = along(mine, 1), along(mine, 2)
    b1, b2 = cross(theirs, 1), cross(theirs, 2)
    chunks = [side, a1, a2, b1, b2]
    for _ in range(2):
        a1, a2 = along(a2, 1), along(a1, 2)
        b1, b2 = along(b2, 1), along(b1, 2)
        chunks += [a1, a2, b1, b2]
    chunks += [along(a2, 1), along(b1, 2)]

    pieces = attend(block_order, q, keys, values, chunks)
    recv = lax.all_to_all(pieces, ("y", "xh", "xl", "c"), split_axis=0, concat_axis=0, tiled=True)
    return combine(recv)


def solution(mesh):
    fine = Mesh(mesh.devices.reshape(NZ, NY, 2, 2, 2), ("z", "y", "xh", "xl", "c"))
    seq, head = ("z", "y", "xh"), ("xl", "c")
    in_specs = (P(seq, head), P(seq, head), P(seq, head), P())
    out_specs = (P(seq + head, None), P(head, seq))
    return jax.shard_map(local, mesh=fine, in_specs=in_specs, out_specs=out_specs, check_vma=False)
```
